32 devices in a mesh: space: 32 (over z, y, x, core).
Axes of the slice: x: 2, y: 2, z: 4, core: 2. Of those that a mesh axis runs over, the one named last changes fastest.
Arguments:
- state: float32 [32768, 1024], P('space'), may hold values from -6 to 6
- obs_value: float32 [16384], P('space'), may hold values from -6 to 6
- obs_sigma: float32 [16384], P('space'), may hold values from 0.3 to 1.5
- obs_noise: float32 [16384, 1024], P('space'), may hold values from -6 to 6
- obs_pos: int32 [2, 16384], P(None, 'space'), may hold values from 0 to 255, as said below
- obs_side: int32 [16384], P('space'), may hold values from 0 to 1
Outputs:
- predicted_states: float32 [32768, 1024], P('space')
The draws below stay inside these ranges and needn't reach their ends.
Inputs may be any that keep to these rules, and one draw needn't show every extreme that they name: `obs_pos`: observation o lies in grid row (o // 512) * 4 plus 0 to 3; its column is 0 to 255.
All inputs are finite; a program needn't handle non-finite values.
Results may differ from the reference program's by a relative error of at most 0.0038.
Values may be sent and summed in bfloat16 or wider, within the bound.
A program may use at most 128 MiB of HBM per device.

```python
import math
import jax
import jax.numpy as jnp
from jax import lax

M = 1024
MESH_WIDTH = 256
ROWS_DEV = 4
OBS_DEV = 512
REACH = 4
CELL_DEV = 1024
CELLS = 32768
OBS = 16384
N_SPACE = 32


def draw_obs_pos(key, part):
    first_key, second_key = jax.random.split(jax.random.fold_in(key, 17))
    block_number = jnp.arange(OBS, dtype=jnp.int32) // OBS_DEV
    obs_row = block_number * ROWS_DEV + jax.random.randint(first_key, (OBS,), 0, ROWS_DEV)
    obs_col = jax.random.randint(second_key, (OBS,), 0, MESH_WIDTH)
    return jnp.stack([obs_row, obs_col]).astype(jnp.int32)


def place_ends(entries, rng, least, largest):
    shape = entries.shape
    index_at = [jax.random.randint(jax.random.fold_in(rng, axis), (), 0, shape[axis]) for axis in range(len(shape))]
    entries = entries.at[tuple(index_at)].set(least)
    longest = shape.index(max(shape))
    index_at[longest] = (index_at[longest] + 1) % shape[longest]
    return entries.at[tuple(index_at)].set(largest)


def steps_of(stream_key, dims, cuts, least, top_value):
    factor_of = 1.0
    for position, shards_of in cuts:
        draws = jax.random.uniform(jax.random.fold_in(jax.random.fold_in(stream_key, 6), position), (shards_of,), jnp.float32, least / len(cuts), top_value / len(cuts))
        factor_of = factor_of * jnp.repeat(jnp.exp(draws), dims[position] // shards_of).reshape((-1,) + (1,) * (len(dims) - 1 - position))
    return factor_of


def bell_draw(rng, dims, deviation, most, cuts=(), held_as=jnp.bfloat16):
    entries = jax.random.normal(rng, dims, jnp.float32) * deviation
    if len(cuts) > 0:
        entries = steps_of(rng, dims, cuts, -0.22, 0.18) * entries
    return jnp.clip(entries, min=-most, max=most).astype(held_as)


def setup_inputs(seed: int = 0) -> dict:
    streams_of = jax.random.split(jax.random.key(seed), 7)
    return {
        "state": bell_draw(streams_of[0], (CELLS, M), 1.0, 6.0, ((0, 32),), jnp.float32),
        "obs_value": bell_draw(streams_of[1], (OBS,), 1.0, 6.0, ((0, 32),), jnp.float32),
        "obs_sigma": jnp.clip(jnp.exp(math.log(1.5) - 1.60943787 * jax.random.uniform(streams_of[2], (OBS,), jnp.float32) ** steps_of(streams_of[2], (OBS,), ((0, 32),), -0.2, 0.2)), 0.3, 1.5),
        "obs_noise": bell_draw(streams_of[3], (OBS, M), 1.0, 6.0, ((0, 32),), jnp.float32),
        "obs_pos": draw_obs_pos(jax.random.fold_in(streams_of[6], 71), 0),
        "obs_side": place_ends(jax.random.randint(streams_of[5], (OBS,), 0, 2), jax.random.fold_in(streams_of[5], 1), 0, 1).astype(jnp.int32),
    }


def gaspari(scaled):
    safe = jnp.maximum(scaled, 1.0)
    near_part = -0.25 * scaled ** 5 + 0.5 * scaled ** 4 + 0.625 * scaled ** 3 - 5.0 / 3.0 * scaled ** 2 + 1.0
    far_part = scaled ** 5 / 12.0 - 0.5 * scaled ** 4 + 0.625 * scaled ** 3 + 5.0 / 3.0 * scaled ** 2 - 5.0 * scaled + 4.0 - 2.0 / (3.0 * safe)
    return jnp.where(scaled <= 1.0, near_part, jnp.where(scaled <= 2.0, far_part, 0.0 * scaled))

def contribution(running_sum, state_anom, cell_row, cell_col, obs_anom, weights, obs_pos, mesh_height, sample_states):
    row_gap = jnp.abs(cell_row[:, None] - obs_pos[0][None, :])
    row_gap = jnp.minimum(row_gap, mesh_height - row_gap)
    col_gap = jnp.abs(cell_col[:, None] - obs_pos[1][None, :])
    col_gap = jnp.minimum(col_gap, MESH_WIDTH - col_gap)
    radius = 1.0 * REACH * ROWS_DEV
    scaled = jnp.sqrt((row_gap * row_gap + col_gap * col_gap).astype(jnp.float32)) / radius
    tapers = jnp.where(row_gap <= REACH * ROWS_DEV, gaspari(scaled), 0.0 * scaled)
    covariance = lax.dot_general(state_anom, obs_anom, (((1,), (1,)), ((), ())), preferred_element_type=jnp.float32)
    gain_block = (tapers * covariance / (sample_states - 1)).astype(jnp.bfloat16)
    return running_sum + jnp.dot(gain_block, weights, preferred_element_type=jnp.float32)

def advance_model(state_mesh_entries, row_above, row_below):
    col_right = jnp.roll(state_mesh_entries, -1, axis=1)
    col_left = jnp.roll(state_mesh_entries, 1, axis=1)
    advect_state = 0.05 * state_mesh_entries * (row_above - row_below + (col_right - col_left))
    diffuse_state = 0.2 * (row_above + row_below + col_right + col_left - 4.0 * state_mesh_entries)
    return state_mesh_entries - advect_state + diffuse_state

def reference(state, obs_value, obs_sigma, obs_noise, obs_pos, obs_side):
    sample_states = state.shape[1]
    mesh_height = ROWS_DEV * N_SPACE
    member_mean = lax.optimization_barrier(jnp.mean(state, axis=1, keepdims=True))
    state_anom = (state - member_mean).astype(jnp.bfloat16)
    obs_row = obs_pos[0]
    obs_col = obs_pos[1]
    partner_col = (obs_col + 2 * obs_side - 1) % MESH_WIDTH
    observed = 0.5 * (state[obs_row * MESH_WIDTH + obs_col] + state[obs_row * MESH_WIDTH + partner_col])
    obs_dev = observed - lax.optimization_barrier(jnp.mean(observed, axis=1, keepdims=True))
    obs_anom = obs_dev.astype(jnp.bfloat16)
    spread = lax.optimization_barrier(jnp.sum(obs_dev * obs_dev, axis=1)) / (sample_states - 1)
    innovation = obs_value[:, None] + obs_sigma[:, None] * obs_noise - observed
    weights = (innovation / (spread + obs_sigma * obs_sigma)[:, None]).astype(jnp.bfloat16)
    anom_blocks = obs_anom.reshape(N_SPACE, OBS_DEV, sample_states)
    weight_blocks = weights.reshape(N_SPACE, OBS_DEV, sample_states)
    pos_blocks = obs_pos.reshape(2, N_SPACE, OBS_DEV).transpose(1, 0, 2)
    local_cells = jnp.arange(CELL_DEV, dtype=jnp.int32)

    def block_increment(block_index):
        slab_anom = lax.dynamic_slice_in_dim(state_anom, (block_index * CELL_DEV).astype(jnp.int32), CELL_DEV, 0)
        cell_row = block_index * ROWS_DEV + local_cells // MESH_WIDTH
        cell_col = local_cells % MESH_WIDTH
        running_sum = jnp.zeros((CELL_DEV, sample_states), jnp.float32)
        for offset in range(-REACH, REACH + 1):
            source = ((block_index + offset) % N_SPACE).astype(jnp.int32)
            running_sum = contribution(running_sum, slab_anom, cell_row, cell_col, anom_blocks[source], weight_blocks[source], pos_blocks[source], mesh_height, sample_states)
        return running_sum
    increments = lax.map(block_increment, jnp.arange(N_SPACE, dtype=jnp.int32))
    analysis = state + increments.reshape(mesh_height * MESH_WIDTH, sample_states)
    state_mesh_entries = analysis.reshape(mesh_height, MESH_WIDTH, sample_states)
    predicted_states = advance_model(state_mesh_entries, jnp.roll(state_mesh_entries, -1, axis=0), jnp.roll(state_mesh_entries, 1, axis=0))
    return predicted_states.reshape(mesh_height * MESH_WIDTH, sample_states)
```

```python
import functools

import jax
import jax.numpy as jnp
from jax import lax
from jax.experimental import pallas as pl
from jax.experimental.pallas import tpu as pltpu
from jax.sharding import PartitionSpec as P

MESH_WIDTH = 256
ROWS_DEV = 4
REACH = 4
POS_ROWS = 16
MESH = pl.DeviceIdType.MESH

OWN, X, Y, Z, D, SO, SX, ST, SD = range(9)
ORDER = [
    (OWN, 0), (OWN, 1), (SO, 0), (SO, 1), (X, 0), (Y, 0), (SX, 0), (X, 1), (Y, 1),
    (Z, 0), (SX, 1), (ST, 0), (D, 0), (Z, 1), (ST, 1), (SD, 0), (D, 1), (SD, 1),
]
AT = {unit: i for i, unit in enumerate(ORDER)}
RELAY = len(ORDER)


def analysis_kernel(
    n, state_ref, own_ref, out_ref, halo_out, anom, pk, edge, halo,
    load_sem, send_sem, recv_sem, edge_send, edge_recv,
):
    width = MESH_WIDTH
    members = state_ref.shape[1]
    half_obs = (pk.shape[1] - POS_ROWS) // 2
    me = lax.axis_index("space")
    core = lax.rem(me, 2)
    chip = me // 2
    quad = lax.rem(chip, 4)
    qy = quad // 2
    qx = lax.rem(quad, 2)
    chips = n // 2
    x_peer = me + 2 - 4 * qx
    y_peer = me + 4 - 8 * qy
    sibling = me + 1 - 2 * core
    ahead8, behind8 = lax.rem(me + 8, n), lax.rem(me + n - 8, n)
    ahead, behind = lax.rem(me + 1, n), lax.rem(me + n - 1, n)
    z_to = lax.rem(me + 8 - 16 * qy + n, n)
    relay_to = lax.rem(me + 8 - 16 * qx + n, n)
    inner = qx + qy == 1

    barrier = pltpu.get_barrier_semaphore()
    for peer in (x_peer, y_peer, ahead8, behind8, ahead, behind):
        pl.semaphore_signal(barrier, inc=1, device_id=(peer,), device_id_type=MESH)
    loads = [
        pltpu.make_async_copy(own_ref.at[h], pk.at[AT[(OWN, h)]], load_sem.at[h]) for h in (0, 1)
    ]
    for load in loads:
        load.start()
    pl.semaphore_wait(barrier, 6)

    sends = []

    def copy(src, dst, peer, new=True, sem=None):
        if sem is None:
            sem = len(sends)
            sends.append((src, dst, peer))
        return pltpu.make_async_remote_copy(
            src_ref=pk.at[src], dst_ref=pk.at[dst], send_sem=send_sem.at[sem],
            recv_sem=recv_sem.at[dst], device_id=(peer,), device_id_type=MESH,
        )

    def arrived(dst):
        pltpu.make_async_remote_copy(
            src_ref=pk.at[dst], dst_ref=pk.at[dst], send_sem=send_sem.at[0],
            recv_sem=recv_sem.at[dst], device_id=(sibling,), device_id_type=MESH,
        ).wait_recv()

    for h in (0, 1):
        loads[h].wait()
        own = AT[(OWN, h)]
        copy(own, AT[(X, h)], x_peer).start()
        copy(own, AT[(Y, h)], y_peer).start()
        copy(own, AT[(SO, h)], sibling).start()

    for r in range(ROWS_DEV):
        rows = pl.ds(r * width, width)
        block = state_ref[rows, :]
        mean = jnp.sum(block, axis=1, keepdims=True) / members
        anom[rows, :] = (block - mean).astype(jnp.bfloat16)
        out_ref[rows, :] = block

    shares_y = qy == core
    n_start = len(sends)
    to_z = {h: n_start + h for h in (0, 1)}
    to_sib = {s: [n_start + 2 + 2 * i + h for h in (0, 1)] for i, s in enumerate((SX, ST, SD))}
    to_d = [n_start + 8, n_start + 9]
    to_relay = n_start + 10

    def got_x(h):
        arrived(AT[(X, h)])
        copy(AT[(X, h)], AT[(SX, h)], sibling, sem=to_sib[SX][h]).start()
        if h == 1:

            @pl.when(inner)
            def _():
                copy(AT[(X, 1)], RELAY, relay_to, sem=to_relay).start()

            @pl.when(jnp.logical_not(inner))
            def _():
                copy(AT[(X, 1)], AT[(D, 1)], y_peer, sem=to_d[1]).start()

    def got_y(h):
        arrived(AT[(Y, h)])
        copy(AT[(Y, h)], AT[(Z, h)], z_to, sem=to_z[h]).start()
        if h == 0:

            @pl.when(jnp.logical_not(inner))
            def _():
                copy(AT[(Y, 0)], AT[(D, 0)], x_peer, sem=to_d[0]).start()

        @pl.when(shares_y)
        def _():
            copy(AT[(Y, h)], AT[(ST, h)], sibling, sem=to_sib[ST][h]).start()

    def got_z(h):
        arrived(AT[(Z, h)])
        if h == 0:

            @pl.when(inner)
            def _():
                copy(AT[(Z, 0)], AT[(D, 0)], x_peer, sem=to_d[0]).start()

        @pl.when(jnp.logical_not(shares_y))
        def _():
            copy(AT[(Z, h)], AT[(ST, h)], sibling, sem=to_sib[ST][h]).start()

    def got_relay():
        @pl.when(inner)
        def _():
            arrived(RELAY)
            copy(RELAY, AT[(D, 1)], y_peer, sem=to_d[1]).start()

    def got_d(h):
        arrived(AT[(D, h)])
        copy(AT[(D, h)], AT[(SD, h)], sibling, sem=to_sib[SD][h]).start()

    def halos():
        low = pltpu.make_async_remote_copy(
            src_ref=edge.at[0], dst_ref=halo.at[1], send_sem=edge_send.at[0],
            recv_sem=edge_recv.at[1], device_id=(behind,), device_id_type=MESH,
        )
        high = pltpu.make_async_remote_copy(
            src_ref=edge.at[1], dst_ref=halo.at[0], send_sem=edge_send.at[1],
            recv_sem=edge_recv.at[0], device_id=(ahead,), device_id_type=MESH,
        )
        return low, high

    def send_halos():
        edge[0] = out_ref[pl.ds(0, width), :].astype(jnp.bfloat16)
        edge[1] = out_ref[pl.ds((ROWS_DEV - 1) * width, width), :].astype(jnp.bfloat16)
        for c in halos():
            c.start()

    events = {}
    for h in (0, 1):
        events.setdefault(AT[(SO, h)], []).append(functools.partial(arrived, AT[(SO, h)]))
        events.setdefault(AT[(X, h)], []).extend(
            [functools.partial(got_x, h), functools.partial(got_y, h)]
        )
        events.setdefault(AT[(Z, h)], []).append(functools.partial(got_z, h))
        events.setdefault(AT[(D, h)], []).append(functools.partial(got_d, h))
        for s in (SX, ST, SD):
            events.setdefault(AT[(s, h)], []).append(functools.partial(arrived, AT[(s, h)]))
    events[AT[(Z, 1)]].insert(0, got_relay)

    def wrap(c):
        return lax.rem(c + chips, chips)

    chip_of = {
        OWN: chip, X: chip + 1 - 2 * qx, Y: chip + 2 - 4 * qy, Z: wrap(chip - 2 + 4 * qy),
        D: wrap(chip - 1 + 2 * qx), ST: wrap(chip - 2 + 4 * core),
    }
    chip_of.update({SO: chip_of[OWN], SX: chip_of[X], SD: chip_of[D]})
    slab_of = {s: 2 * chip_of[s] + (core if s <= D else 1 - core) for s in range(9)}
    height = 1.0 * ROWS_DEV * n
    radius = 1.0 * REACH * ROWS_DEV
    last = len(ORDER) - 1

    def step(t, carry):
        u = t // ROWS_DEV
        j = lax.rem(t, ROWS_DEV)
        for unit, todo in events.items():

            @pl.when(t == unit * ROWS_DEV)
            def _(todo=todo):
                for do in todo:
                    do()

        @pl.when(t == last * ROWS_DEV + 2)
        def _():
            send_halos()

        row = jnp.where(j < 2, (ROWS_DEV - 1) * j, j - 1)
        source = slab_of[ORDER[0][0]]
        for i in range(1, len(ORDER)):
            source = jnp.where(u == i, slab_of[ORDER[i][0]], source)
        place = pk[u, pl.ds(2 * half_obs, POS_ROWS), :].astype(jnp.float32)[0:1, :]
        obs_row = place[:, :half_obs] + (ROWS_DEV * source).astype(jnp.float32)
        obs_col = place[:, half_obs : 2 * half_obs]
        cell_row = (ROWS_DEV * me + row).astype(jnp.float32)
        row_gap = jnp.abs(cell_row - obs_row)
        row_gap = jnp.minimum(row_gap, height - row_gap)
        row_part = jnp.where(row_gap <= radius, row_gap * row_gap, 9.0 * radius * radius)
        cell_col = lax.broadcasted_iota(jnp.int32, (width, half_obs), 0).astype(jnp.float32)
        col_gap = jnp.abs(cell_col - obs_col)
        col_gap = jnp.minimum(col_gap, width - col_gap)
        squared = col_gap * col_gap + row_part
        inverse = lax.rsqrt(jnp.maximum(squared, 0.25))
        z = squared * inverse * (1.0 / radius)
        near = 1.0 + z * z * (-5.0 / 3.0 + z * (0.625 + z * (0.5 - 0.25 * z)))
        far = 4.0 - (2.0 / 3.0 * radius) * inverse + z * (
            -5.0 + z * (5.0 / 3.0 + z * (0.625 + z * (-0.5 + z * (1.0 / 12.0))))
        )
        taper = jnp.where(z <= 1.0, near, jnp.where(z <= 2.0, far, 0.0))
        rows = pl.ds(pl.multiple_of(row * width, width), width)
        covariance = lax.dot_general(
            anom[rows, :], pk[u, pl.ds(0, half_obs), :], (((1,), (1,)), ((), ())),
            preferred_element_type=jnp.float32,
        )
        gain = (taper * covariance * (1.0 / (members - 1))).astype(jnp.bfloat16)
        out_ref[rows, :] += jnp.dot(
            gain, pk[u, pl.ds(half_obs, half_obs), :], preferred_element_type=jnp.float32
        )
        return carry

    lax.fori_loop(0, len(ORDER) * ROWS_DEV, step, 0)

    for c in halos():
        c.wait()
    halo_out[...] = halo[...]
    for i, (src, dst, peer) in enumerate(sends[:n_start]):
        copy(src, dst, peer, sem=i).wait_send()
    for sem in [*to_z.values(), *sum(to_sib.values(), []), *to_d]:
        copy(0, 0, sibling, sem=sem).wait_send()

    @pl.when(inner)
    def _():
        copy(0, 0, sibling, sem=to_relay).wait_send()


def forecast_kernel(a_ref, halo_ref, out_ref):
    width = MESH_WIDTH
    for r in range(ROWS_DEV):
        a = a_ref[pl.ds(r * width, width), :]
        if r + 1 < ROWS_DEV:
            above = a_ref[pl.ds((r + 1) * width, width), :]
        else:
            above = halo_ref[1].astype(jnp.float32)
        if r > 0:
            below = a_ref[pl.ds((r - 1) * width, width), :]
        else:
            below = halo_ref[0].astype(jnp.float32)
        right = pltpu.roll(a, width - 1, 0)
        left = pltpu.roll(a, 1, 0)
        advect = 0.05 * a * (above - below + (right - left))
        diffuse = 0.2 * (above + below + right + left - 4.0 * a)
        out_ref[pl.ds(r * width, width), :] = a - advect + diffuse


def on_device(n, state, obs_value, obs_sigma, obs_noise, obs_pos, obs_side):
    cells, members = state.shape
    obs = obs_value.shape[0]
    half = obs // 2
    device = lax.axis_index("space")
    local_row = obs_pos[0] - device * ROWS_DEV
    obs_col = obs_pos[1]
    partner_col = (obs_col + 2 * obs_side - 1) % MESH_WIDTH
    observed = 0.5 * (
        state[local_row * MESH_WIDTH + obs_col] + state[local_row * MESH_WIDTH + partner_col]
    )
    obs_dev = observed - jnp.mean(observed, axis=1, keepdims=True)
    obs_anom = obs_dev.astype(jnp.bfloat16)
    spread = jnp.sum(obs_dev * obs_dev, axis=1) / (members - 1)
    innovation = obs_value[:, None] + obs_sigma[:, None] * obs_noise - observed
    weights = (innovation / (spread + obs_sigma * obs_sigma)[:, None]).astype(jnp.bfloat16)
    place = jnp.stack([local_row, obs_col]).astype(jnp.bfloat16)
    place = place.reshape(2, 2, half).transpose(1, 0, 2).reshape(2, 1, obs)
    place = jnp.pad(place, ((0, 0), (0, POS_ROWS - 1), (0, members - obs)))
    own = jnp.concatenate(
        [obs_anom.reshape(2, half, members), weights.reshape(2, half, members), place], axis=1
    )
    units = len(ORDER)
    vmem = pl.BlockSpec(memory_space=pltpu.VMEM)
    analysis, halo = pl.pallas_call(
        functools.partial(analysis_kernel, n),
        out_shape=(
            jax.ShapeDtypeStruct((cells, members), jnp.float32),
            jax.ShapeDtypeStruct((2, MESH_WIDTH, members), jnp.bfloat16),
        ),
        in_specs=[vmem, pl.BlockSpec(memory_space=pl.ANY)],
        out_specs=(vmem, vmem),
        scratch_shapes=[
            pltpu.VMEM((cells, members), jnp.bfloat16),
            pltpu.VMEM((units + 1, obs + POS_ROWS, members), jnp.bfloat16),
            pltpu.VMEM((2, MESH_WIDTH, members), jnp.bfloat16),
            pltpu.VMEM((2, MESH_WIDTH, members), jnp.bfloat16),
            pltpu.SemaphoreType.DMA((2,)),
            pltpu.SemaphoreType.DMA((17,)),
            pltpu.SemaphoreType.DMA((units + 1,)),
            pltpu.SemaphoreType.DMA((2,)),
            pltpu.SemaphoreType.DMA((2,)),
        ],
        compiler_params=pltpu.CompilerParams(
            collective_id=0, has_side_effects=True, vmem_limit_bytes=56 * 2**20
        ),
        name="analysis",
    )(state, own)
    lanes = 128
    return pl.pallas_call(
        forecast_kernel,
        grid=(members // lanes,),
        out_shape=jax.ShapeDtypeStruct((cells, members), jnp.float32),
        in_specs=[
            pl.BlockSpec((cells, lanes), lambda m: (0, m)),
            pl.BlockSpec((2, MESH_WIDTH, lanes), lambda m: (0, 0, m)),
        ],
        out_specs=pl.BlockSpec((cells, lanes), lambda m: (0, m)),
        name="forecast",
    )(analysis, halo)


def solution(mesh):
    placed = (
        P("space", None),
        P("space"),
        P("space"),
        P("space", None),
        P(None, "space"),
        P("space"),
    )
    return jax.shard_map(
        functools.partial(on_device, mesh.shape["space"]),
        mesh=mesh, in_specs=placed, out_specs=P("space", None), check_vma=False,
    )
```
